32 devices in a mesh: dp: 32 (over z, y, x, core).
Axes of the slice: x: 2, y: 2, z: 4, core: 2. Of those that a mesh axis runs over, the one named last changes fastest.
Arguments:
- captions: bfloat16 [1024, 77, 768], P('dp'), may hold values from -6 to 6
- caption_layout: int32 [2, 1024], replicated, may hold values from 0 to 77, as said below
- images: bfloat16 [1024, 768], P('dp'), may hold values from -0.24 to 0.24
- w_query: bfloat16 [768, 768], replicated, may hold values from -0.21875 to 0.21875
- w_keyval: bfloat16 [768, 1536], replicated, may hold values from -0.21875 to 0.21875
- w_out: bfloat16 [768, 768], replicated, may hold values from -0.21875 to 0.21875
- w_up: bfloat16 [768, 3072], replicated, may hold values from -0.21875 to 0.21875
- w_down: bfloat16 [3072, 768], replicated, may hold values from -0.109375 to 0.109375
- w_proj: bfloat16 [768, 768], replicated, may hold values from -0.009114583 to 0.009114583
Outputs:
- image_grad: float32 [1024, 768], P('dp')
- text_grad: float32 [1024, 768], P('dp')
The draws below stay inside these ranges and needn't reach their ends.
Inputs may be any that keep to these rules, and one draw needn't show every extreme that they name: `caption_layout`: row 0 holds each caption's token count; row 1 is 1 where the caption is encoded by the next index of dp (index 0 after the last) and 0 where by its own. Exactly 8 of each device's captions carry 1. The captions one device encodes (its own that carry 0 and those carrying 1 of the index before it) hold at most 2048 tokens together, exactly that many on some device.
All inputs are finite; a program needn't handle non-finite values.
Results may differ from the reference program's by a relative error of at most 0.018.
Values may be sent and summed in bfloat16 or wider, within the bound.
No kernel may reach another device: no remote copies, remote signals or barrier semaphores. Data moves between devices by JAX's collectives and lax.ppermute only.
A program may use at most 128 MiB of HBM per device.

```python
import math
import jax
import jax.numpy as jnp
from jax import lax

D = 768
HEADS = 12
FF = 3072
E = 768
CTX = 77
CAP_DEV = 32
HAND = 8
TOK_CAP = 2048
PAIRS = 1024
N_DP = 32


def caption_plan(key):
    order_key = jax.random.fold_in(key, 7102)
    length_key = jax.random.fold_in(key, 7103)
    heavy_key = jax.random.fold_in(key, 7104)
    hand_counts = jnp.full((N_DP,), HAND, jnp.int32)
    permuted = jax.vmap(lambda sub_key: jax.random.permutation(sub_key, CAP_DEV))(jax.random.split(order_key, N_DP))
    position_rank = jnp.argsort(permuted, axis=1)
    handed_flags = (position_rank < hand_counts[:, None]).astype(jnp.int32)
    owner_index = jnp.broadcast_to(jnp.arange(N_DP, dtype=jnp.int32)[:, None], (N_DP, CAP_DEV))
    group_index = ((owner_index + handed_flags) % N_DP).reshape(-1)
    heaviness = jax.random.randint(heavy_key, (N_DP, 1), 2, 5)
    raw_length = (jax.random.randint(length_key, (N_DP, CAP_DEV), 0, CTX) * heaviness // 4).reshape(-1)
    raw_length = jnp.where(group_index == 0, CTX - 1, raw_length)
    onehot = (group_index[:, None] == jnp.arange(N_DP, dtype=jnp.int32)[None, :]).astype(jnp.int32)
    members = jnp.sum(onehot, axis=0)
    total_raw = jnp.sum(onehot * raw_length[:, None], axis=0)
    room_left = TOK_CAP - members
    own_room = room_left[group_index]
    own_total = jnp.maximum(total_raw[group_index], 1)
    floor_part = raw_length * own_room // own_total
    floor_total = jnp.sum(onehot * floor_part[:, None], axis=0)
    group_rank = jnp.sum((jnp.cumsum(onehot, axis=0) - onehot) * onehot, axis=1)
    extra_token = (group_rank < (room_left - floor_total)[group_index]).astype(jnp.int32)
    scaled = (total_raw > room_left)[group_index]
    lengths = jnp.where(scaled, 1 + floor_part + extra_token, 1 + raw_length)
    return jnp.stack([lengths, handed_flags.reshape(-1)]).astype(jnp.int32)


def draw_caption_layout(key, part):
    return caption_plan(key)


def draw_captions(key, part):
    noise = jax.random.normal(jax.random.fold_in(key, 7211), (PAIRS, CTX, D), jnp.float32)
    values = jnp.clip(noise, -6.0, 6.0)
    return values.astype(jnp.bfloat16)


def draw_w_proj(key, part):
    noise = jax.random.normal(jax.random.fold_in(key, 7221), (D, E), jnp.float32)
    values = jnp.clip(noise, -6.0, 6.0) / math.sqrt(D * E)
    return values.astype(jnp.bfloat16)


def draw_images(key, part):
    noise = jax.random.normal(jax.random.fold_in(key, 7231), (PAIRS, E), jnp.float32)
    values = 0.04 * jnp.clip(noise, -5.9, 5.9)
    return values.astype(jnp.bfloat16)


def bell_draw(key, dims, scale, most, held_as=jnp.bfloat16):
    values = jax.random.normal(key, dims, jnp.float32) * scale
    return jnp.minimum(jnp.maximum(values, -most), most).astype(held_as)


def setup_inputs(seed: int = 0) -> dict:
    seeds = jax.random.split(jax.random.key(seed), 10)
    captions = draw_captions(jax.random.fold_in(seeds[9], 71), 0)
    caption_layout = draw_caption_layout(jax.random.fold_in(seeds[9], 71), 0)
    images = draw_images(jax.random.fold_in(seeds[9], 71), 0)
    w_query = bell_draw(seeds[3], (D, D), D ** -0.5, 0.21875)
    w_keyval = bell_draw(seeds[4], (D, 2 * D), D ** -0.5, 0.21875)
    w_out = bell_draw(seeds[5], (D, D), D ** -0.5, 0.21875)
    w_up = bell_draw(seeds[6], (D, FF), D ** -0.5, 0.21875)
    w_down = bell_draw(seeds[7], (FF, D), FF ** -0.5, 0.109375)
    w_proj = draw_w_proj(jax.random.fold_in(seeds[9], 71), 0)
    return dict(captions=captions, caption_layout=caption_layout, images=images, w_query=w_query, w_keyval=w_keyval, w_out=w_out, w_up=w_up, w_down=w_down, w_proj=w_proj)


LOGIT_SCALE = 100.0
EPS_NORM = 1e-05
EPS_UNIT = 1e-06

def layer_norm(values):
    values = values.astype(jnp.float32)
    center = values - lax.optimization_barrier(jnp.mean(values, axis=-1, keepdims=True))
    spread = lax.optimization_barrier(jnp.mean(center * center, axis=-1, keepdims=True))
    return center * lax.rsqrt(spread + EPS_NORM)

def unit_rows(values):
    values = values.astype(jnp.float32)
    return values * lax.rsqrt(lax.optimization_barrier(jnp.sum(values * values, axis=-1, keepdims=True)) + EPS_UNIT)

def contract_first(left, right):
    return lax.dot_general(left, right, (((0,), (0,)), ((), ())), preferred_element_type=jnp.float32)

def contract_last(left, right):
    return lax.dot_general(left, right, (((1,), (1,)), ((), ())), preferred_element_type=jnp.float32)

def reference(captions, caption_layout, images, w_query, w_keyval, w_out, w_up, w_down, w_proj):
    model_width = captions.shape[2]
    head_dim = model_width // HEADS

    def encode_block(block_item):
        caption_block, block_lengths = block_item
        block_count = caption_block.shape[0]
        normed = layer_norm(caption_block).astype(jnp.bfloat16)
        keyval = jnp.dot(normed.reshape(-1, model_width), w_keyval, preferred_element_type=jnp.float32)
        keyval = keyval.astype(jnp.bfloat16).reshape(block_count, CTX, 2 * model_width)
        last_slot = (block_lengths - 1).astype(jnp.int32)[:, None, None]
        end_normed = jnp.take_along_axis(normed, last_slot, axis=1)[:, 0]
        end_tokens = jnp.take_along_axis(caption_block, last_slot, axis=1)[:, 0]
        query = jnp.dot(end_normed, w_query, preferred_element_type=jnp.float32).astype(jnp.bfloat16)
        key_heads = keyval[:, :, :model_width].reshape(block_count, CTX, HEADS, head_dim).astype(jnp.float32)
        value_heads = keyval[:, :, model_width:].reshape(block_count, CTX, HEADS, head_dim).astype(jnp.float32)
        query_heads = query.reshape(block_count, HEADS, head_dim).astype(jnp.float32)
        scores = jnp.einsum('chd,cthd->cht', query_heads, key_heads) / math.sqrt(head_dim)
        inside = jnp.arange(CTX)[None, None, :] < block_lengths[:, None, None]
        masked = jnp.where(inside, scores, -jnp.inf)
        peak = lax.optimization_barrier(jnp.max(masked, axis=-1, keepdims=True))
        exponent = jnp.exp(masked - peak)
        attention = (exponent / lax.optimization_barrier(jnp.sum(exponent, axis=-1, keepdims=True))).astype(jnp.bfloat16)
        mixed_heads = jnp.einsum('cht,cthd->chd', attention.astype(jnp.float32), value_heads)
        mixed_heads = mixed_heads.astype(jnp.bfloat16).reshape(block_count, model_width)
        residual = end_tokens.astype(jnp.float32) + jnp.dot(mixed_heads, w_out, preferred_element_type=jnp.float32)
        residual = residual.astype(jnp.bfloat16)
        inner_norm = layer_norm(residual).astype(jnp.bfloat16)
        hidden = jax.nn.gelu(jnp.dot(inner_norm, w_up, preferred_element_type=jnp.float32), approximate=False)
        hidden = hidden.astype(jnp.bfloat16)
        final_rows = residual.astype(jnp.float32) + jnp.dot(hidden, w_down, preferred_element_type=jnp.float32)
        pooled = layer_norm(final_rows).astype(jnp.bfloat16)
        return jnp.dot(pooled, w_proj, preferred_element_type=jnp.float32).astype(jnp.bfloat16)
    caption_blocks = captions.reshape(N_DP, CAP_DEV, CTX, model_width)
    length_blocks = caption_layout[0].reshape(N_DP, CAP_DEV)
    text_embed = lax.map(encode_block, (caption_blocks, length_blocks)).reshape(PAIRS, -1)
    image_unit = unit_rows(images).astype(jnp.bfloat16)
    text_unit = unit_rows(text_embed).astype(jnp.bfloat16)
    scores = LOGIT_SCALE * contract_last(image_unit, text_unit)
    row_peak = lax.optimization_barrier(jnp.max(scores, axis=1, keepdims=True))
    row_logsum = row_peak[:, 0] + jnp.log(lax.optimization_barrier(jnp.sum(jnp.exp(scores - row_peak), axis=1)))
    column_peak = lax.optimization_barrier(jnp.max(scores, axis=0, keepdims=True))
    column_logsum = column_peak[0] + jnp.log(lax.optimization_barrier(jnp.sum(jnp.exp(scores - column_peak), axis=0)))
    row_weights = jnp.exp(scores - row_logsum[:, None]).astype(jnp.bfloat16)
    column_weights = jnp.exp(scores - column_logsum[None, :]).astype(jnp.bfloat16)
    half_scale = 0.5 * LOGIT_SCALE
    image_unit_grad = half_scale * (jnp.dot(row_weights, text_unit, preferred_element_type=jnp.float32) + jnp.dot(column_weights, text_unit, preferred_element_type=jnp.float32))
    image_unit_grad = image_unit_grad - LOGIT_SCALE * text_unit.astype(jnp.float32)
    text_unit_grad = half_scale * (contract_first(row_weights, image_unit) + contract_first(column_weights, image_unit))
    text_unit_grad = text_unit_grad - LOGIT_SCALE * image_unit.astype(jnp.float32)
    image_value, image_back = jax.vjp(unit_rows, images.astype(jnp.float32))
    text_value, text_back = jax.vjp(unit_rows, text_embed.astype(jnp.float32))
    return (image_back(image_unit_grad)[0], text_back(text_unit_grad)[0])
```

```python
import functools
import math

import jax
import jax.numpy as jnp
from jax import lax
from jax.experimental import pallas as pl
from jax.experimental.pallas import tpu as pltpu
from jax.sharding import PartitionSpec as P

HEADS = 12
HEAD_ROWS = 16
LOGIT_SCALE = 100.0
EPS_NORM = 1e-05
EPS_UNIT = 1e-06
BF16 = jnp.bfloat16
F32 = jnp.float32
VMEM_LIMIT = 60 * 1024 * 1024


def layer_norm(values):
    center = values - jnp.mean(values, axis=-1, keepdims=True)
    spread = jnp.mean(center * center, axis=-1, keepdims=True)
    return center * lax.rsqrt(spread + EPS_NORM)


def inverse_norm(values):
    return lax.rsqrt(jnp.sum(values * values, axis=-1, keepdims=True) + EPS_UNIT)


def dot(left, right):
    return jnp.dot(left, right, preferred_element_type=F32)


def dot_last(left, right):
    return lax.dot_general(left, right, (((1,), (1,)), ((), ())), preferred_element_type=F32)


def erf(x):
    x = jnp.clip(x, -3.832506856900711, 3.832506856900711)
    y = x * x
    top = jnp.full_like(x, 0.00022905065861350646)
    for c in (
        0.0034082910107109506,
        0.050955695062380861,
        0.18520832239976145,
        1.128379143519084,
    ):
        top = top * y + c
    bottom = jnp.full_like(x, -1.1791602954361697e-7)
    for c in (
        0.000023547966471313185,
        0.0010179625278914885,
        0.014070470171167667,
        0.11098505178285362,
        0.49746925110067538,
        1.0,
    ):
        bottom = bottom * y + c
    return x * top / bottom


def encode_kernel(
    layout_ref, captions_ref, *refs, chunk
):
    (weight_refs, (embed_ref, unit_ref)) = (refs[:6], refs[6:8])
    (caps, normed, last, mapped, score, mix) = refs[8:14]
    weights, cap_sem, weight_sem = refs[14:20], refs[20], refs[21]
    count, context, width = caps.shape
    head_dim = width // HEADS
    base = lax.axis_index("dp") * count

    def cap_copy(i):
        part = pl.ds(i * chunk, chunk)
        return pltpu.make_async_copy(captions_ref.at[part], caps.at[part], cap_sem.at[i])

    def weight_copy(i):
        return pltpu.make_async_copy(weight_refs[i], weights[i], weight_sem.at[i])

    for i in range(count // chunk):
        cap_copy(i).start()
    for i in range(6):
        weight_copy(i).start()
    w_query, w_keyval, w_out, w_up, w_down, w_proj = weights

    row = lax.broadcasted_iota(jnp.int32, (context, width), 0)
    for i in range(count // chunk):
        cap_copy(i).wait()

        def normalise(c, _):
            value = caps[c].astype(F32)
            normed[c] = layer_norm(value).astype(BF16)
            picked = jnp.where(row == layout_ref[0, base + c] - 1, value, 0.0)
            last[pl.ds(c, 1), :] = jnp.sum(picked, axis=0, keepdims=True)
            return _

        lax.fori_loop(i * chunk, (i + 1) * chunk, normalise, 0, unroll=2)

    tokens = last[...]
    weight_copy(0).wait()
    query = dot(layer_norm(tokens).astype(BF16), w_query[...]).astype(BF16).astype(F32)
    shape = (count, HEAD_ROWS, width)
    own_head = (
        lax.broadcasted_iota(jnp.int32, shape, 2) // head_dim
        == lax.broadcasted_iota(jnp.int32, shape, 1)
    )
    spread = jnp.where(own_head, jnp.broadcast_to(query[:, None, :], shape), 0.0)
    spread = spread.reshape(count * HEAD_ROWS, width).astype(BF16)
    weight_copy(1).wait()
    mapped[...] = dot_last(spread, w_keyval[:, :width]).astype(BF16).reshape(shape)

    for c in range(count):
        score[c, :, :context] = dot_last(mapped[c], normed[c])
    position = lax.broadcasted_iota(jnp.int32, (HEAD_ROWS, score.shape[2]), 1)
    scale = 1.0 / math.sqrt(head_dim)
    for c in range(count):
        masked = jnp.where(position < layout_ref[0, base + c], score[c] * scale, -jnp.inf)
        exponent = jnp.exp(masked - jnp.max(masked, axis=-1, keepdims=True))
        attention = exponent / jnp.sum(exponent, axis=-1, keepdims=True)
        score[c] = attention
    for c in range(count):
        mix[c] = dot(score[c, :, :context].astype(BF16), normed[c]).astype(BF16)
    mixed = dot(mix[...].reshape(count * HEAD_ROWS, width), w_keyval[:, width:]).reshape(shape)
    mixed = jnp.sum(jnp.where(own_head, mixed, 0.0), axis=1).astype(BF16)
    weight_copy(2).wait()
    residual = (tokens + dot(mixed, w_out[...])).astype(BF16).astype(F32)
    inner = layer_norm(residual).astype(BF16)
    weight_copy(3).wait()
    hidden = dot(inner, w_up[...])
    hidden = (0.5 * hidden * (1.0 + erf(hidden * math.sqrt(0.5)))).astype(BF16)
    weight_copy(4).wait()
    final = residual + dot(hidden, w_down[...])
    pooled = layer_norm(final).astype(BF16)
    weight_copy(5).wait()
    embed = dot(pooled, w_proj[...]).astype(BF16)
    embed_ref[...] = embed
    embed = embed.astype(F32)
    unit_ref[...] = (embed * inverse_norm(embed)).astype(BF16)


def encode(layout, captions, weights):
    count, context, width = captions.shape
    chunk = 4 if count % 4 == 0 else 1
    joint = weights[5].shape[1]
    result = jax.ShapeDtypeStruct((count, joint), BF16)
    flops = 2 * count * (sum(w.size for w in weights) + 2 * HEAD_ROWS * context * width)
    return pl.pallas_call(
        functools.partial(encode_kernel, chunk=chunk),
        out_shape=(result, result),
        in_specs=[pl.BlockSpec(memory_space=pltpu.SMEM)]
        + [pl.BlockSpec(memory_space=pl.ANY)] * 7,
        out_specs=(pl.BlockSpec(memory_space=pltpu.VMEM),) * 2,
        scratch_shapes=[
            pltpu.VMEM((count, context, width), BF16),
            pltpu.VMEM((count, context, width), BF16),
            pltpu.VMEM((count, width), F32),
            pltpu.VMEM((count, HEAD_ROWS, width), BF16),
            pltpu.VMEM((count, HEAD_ROWS, 128), F32),
            pltpu.VMEM((count, HEAD_ROWS, width), BF16),
        ]
        + [pltpu.VMEM(w.shape, w.dtype) for w in weights]
        + [
            pltpu.SemaphoreType.DMA((count // chunk,)),
            pltpu.SemaphoreType.DMA((6,)),
        ],
        compiler_params=pltpu.CompilerParams(vmem_limit_bytes=VMEM_LIMIT),
        cost_estimate=pl.CostEstimate(
            flops=flops,
            bytes_accessed=2 * (captions.size + sum(w.size for w in weights)),
            transcendentals=count * HEAD_ROWS * 128,
        ),
        name="encode",
    )(layout, captions, *weights)


def unit_grad(grad, value):
    inverse = inverse_norm(value)
    inner = jnp.sum(value * grad, axis=-1, keepdims=True)
    return grad * inverse - value * (inner * inverse * inverse * inverse)


def loss_kernel(images_a, images_b, texts_a, texts_b, embed, image_out, text_out, *scratch, tile):
    unit, sides, row_lse, own_rows = scratch
    half = images_a.shape[0]
    count = embed.shape[0]
    total = 2 * half
    texts = (texts_a, texts_b)
    for h, part in enumerate((images_a, images_b)):

        def normalise(i, _, part=part, h=h):
            value = part[pl.ds(i * tile, tile), :].astype(F32)
            unit[pl.ds(h * half + i * tile, tile), :] = (value * inverse_norm(value)).astype(BF16)
            return _

        lax.fori_loop(0, half // tile, normalise, 0)

    def scores(rows):
        return [LOGIT_SCALE * dot_last(rows, t[...]) for t in texts]

    def step(i, carry):
        rows = pl.ds(i * tile, tile)
        both = scores(unit[rows, :])
        sides[rows, :] = both[0][:, :128]
        peak = jnp.maximum(
            jnp.max(both[0], axis=1, keepdims=True), jnp.max(both[1], axis=1, keepdims=True)
        )
        total_row = jnp.zeros((tile, 1), F32)
        result = []
        for s, (top, mass) in zip(both, carry):
            total_row += jnp.sum(jnp.exp(s - peak), axis=1, keepdims=True)
            higher = jnp.maximum(top, jnp.max(s, axis=0, keepdims=True))
            mass = mass * jnp.exp(top - higher) + jnp.sum(
                jnp.exp(s - higher), axis=0, keepdims=True
            )
            result.append((higher, mass))
        row_lse[rows, :] = jnp.broadcast_to(peak + jnp.log(total_row), (tile, 128))
        return tuple(result)

    start = (jnp.full((1, half), -jnp.inf, F32), jnp.zeros((1, half), F32))
    ends = lax.fori_loop(0, total // tile, step, (start, start))
    column_lse = [top + jnp.log(mass) for top, mass in ends]

    own_unit = unit[:count, :]
    own_row_lse = row_lse[:count, :1]
    grad = -LOGIT_SCALE * texts_a[:count, :].astype(F32)
    for s, lse, t in zip(scores(own_unit), column_lse, texts):
        weights = jnp.concatenate(
            [jnp.exp(s - own_row_lse).astype(BF16), jnp.exp(s - lse).astype(BF16)], axis=0
        )
        both = dot(weights, t[...])
        grad += (0.5 * LOGIT_SCALE) * (both[:count] + both[count:])
    image_out[...] = unit_grad(grad, images_a[:count, :].astype(F32))

    side = sides[...]
    grad = -LOGIT_SCALE * own_unit.astype(F32)
    by_row = jnp.exp(side - row_lse[...]).T[:count].astype(BF16)
    by_column = jnp.exp(side - column_lse[0][:, :128]).T[:count].astype(BF16)
    both = dot(jnp.concatenate([by_row, by_column], axis=0), unit[...])
    grad += (0.5 * LOGIT_SCALE) * (both[:count] + both[count:])
    text_out[...] = unit_grad(grad, embed[...].astype(F32))


def loss(images, texts, embed):
    half, width = images[0].shape
    count = embed.shape[0]
    tile = 128
    result = jax.ShapeDtypeStruct((count, width), F32)
    return pl.pallas_call(
        functools.partial(loss_kernel, tile=tile),
        out_shape=(result, result),
        in_specs=[pl.BlockSpec(memory_space=pltpu.VMEM)] * 5,
        out_specs=(pl.BlockSpec(memory_space=pltpu.VMEM),) * 2,
        scratch_shapes=[
            pltpu.VMEM((2 * half, width), BF16),
            pltpu.VMEM((2 * half, 128), F32),
            pltpu.VMEM((2 * half, 128), F32),
            pltpu.VMEM((8, 128), F32),
        ],
        compiler_params=pltpu.CompilerParams(vmem_limit_bytes=48 * 1024 * 1024),
        cost_estimate=pl.CostEstimate(
            flops=8 * half * half * width, bytes_accessed=8 * half * width, transcendentals=8 * half * half
        ),
        name="loss",
    )(*images, *texts, embed)


def from_partner(value, mask):
    devices = lax.axis_size("dp")
    return lax.ppermute(value, "dp", [(i, i ^ mask) for i in range(devices)])


def digit_masks(devices):
    groups, high = [], devices
    while high > 2:
        low = max(high // 4, 2)
        groups.append([k * low for k in range(1, high // low)])
        high = low
    return groups


def gather_rail(value):
    for masks in digit_masks(lax.axis_size("dp")):
        value = jnp.concatenate([value] + [from_partner(value, m) for m in masks], axis=0)
    return value


def body(captions, layout, images, *weights):
    image_rail = gather_rail(images)
    image_other = from_partner(image_rail, 1)
    embed, unit = encode(layout, captions, weights)
    text_rail = gather_rail(unit)
    text_other = from_partner(text_rail, 1)
    return loss((image_rail, image_other), (text_rail, text_other), embed)


def solution(mesh):
    return jax.shard_map(
        body,
        mesh=mesh,
        in_specs=(P("dp", None, None), P(), P("dp", None), P(), P(), P(), P(), P(), P()),
        out_specs=(P("dp", None), P("dp", None)),
        check_vma=False,
    )
```

```python
import functools
import math

import jax
import jax.numpy as jnp
from jax import lax
from jax.experimental import pallas as pl
from jax.experimental.pallas import tpu as pltpu
from jax.sharding import PartitionSpec as P


HEADS = 12
GROUP = 8
LOGIT_SCALE = 100.0
EPS_NORM = 1e-05
EPS_UNIT = 1e-06
BF16 = jnp.bfloat16
F32 = jnp.float32
MIB = 1024 * 1024
UNIT_FLOPS = 4 * 10**9


def layer_norm(values):
    center = values - jnp.mean(values, axis=-1, keepdims=True)
    spread = jnp.mean(center * center, axis=-1, keepdims=True)
    return center * lax.rsqrt(spread + EPS_NORM)


def inverse_norm(values):
    return lax.rsqrt(jnp.sum(values * values, axis=-1, keepdims=True) + EPS_UNIT)


def dot(left, right):
    return jnp.dot(left, right, preferred_element_type=F32)


def dot_last(left, right):
    return lax.dot_general(left, right, (((1,), (1,)), ((), ())), preferred_element_type=F32)


def erf(x):
    x = jnp.clip(x, -3.832506856900711, 3.832506856900711)
    y = x * x
    top = jnp.full_like(x, 0.00022905065861350646)
    for c in (
        0.0034082910107109506,
        0.050955695062380861,
        0.18520832239976145,
        1.128379143519084,
    ):
        top = top * y + c
    bottom = jnp.full_like(x, -1.1791602954361697e-7)
    for c in (
        0.000023547966471313185,
        0.0010179625278914885,
        0.014070470171167667,
        0.11098505178285362,
        0.49746925110067538,
        1.0,
    ):
        bottom = bottom * y + c
    return x * top / bottom


def attend_kernel(
    layout, caps, w_query, w_keyval, w_out, residual_ref, normed, mapped, mix, key, limits
):
    context, count, width = caps.shape
    groups = count // GROUP
    slots = normed.shape[1]
    head_dim = width // HEADS
    base = lax.axis_index("dp") * count
    lengths = [layout[0, base + c] for c in range(count)]
    ends = [jnp.clip(length - 1, 0, context - 1) for length in lengths]

    rows = GROUP * HEADS
    lane = lax.broadcasted_iota(jnp.int32, (rows, slots), 1)
    line = lax.broadcasted_iota(jnp.int32, (rows, slots), 0)
    key[...] = jnp.where(lane % GROUP == line % GROUP, lane // GROUP, context)
    owner = lax.broadcasted_iota(jnp.int32, (rows, 128), 0) % GROUP
    for g in range(groups):
        limit = jnp.full((rows, 128), 0, jnp.int32)
        for k in range(GROUP):
            limit = jnp.where(owner == k, lengths[g * GROUP + k], limit)
        limits[g] = limit
        normed[g, :, width:] = jnp.ones((slots, 128), BF16)
    pair = 2 * GROUP
    done = (context + 1) // 2 * pair

    def normalise(g):
        for t in range(context // 2):
            value = caps[pl.ds(2 * t, 2), pl.ds(g * GROUP, GROUP)].astype(F32).reshape(pair, width)
            normed[g, pl.ds(t * pair, pair), :width] = layer_norm(value).astype(BF16)
        if context % 2:
            tail = layer_norm(caps[context - 1, pl.ds(g * GROUP, GROUP)].astype(F32))
            tail = jnp.concatenate([tail, jnp.zeros((GROUP, width), F32)], axis=0)
            normed[g, pl.ds(context // 2 * pair, pair), :width] = tail.astype(BF16)
        if done < slots:
            normed[g, pl.ds(done, slots - done), :width] = jnp.zeros((slots - done, width), BF16)

    normalise(0)
    row = lax.broadcasted_iota(jnp.int32, (GROUP, width), 0)
    tokens = []
    for g in range(groups):
        part = pl.ds(g * GROUP, GROUP)
        lines = [caps[ends[g * GROUP + k], part].astype(F32) for k in range(GROUP)]
        token = lines[0]
        for k in range(1, GROUP):
            token = jnp.where(row == k, lines[k], token)
        tokens.append(token)
    tokens = jnp.concatenate(tokens, axis=0)
    end_normed = layer_norm(tokens).astype(BF16)
    query = dot(end_normed, w_query[...]).astype(BF16).astype(F32)
    normalise(1)
    head_of = lax.broadcasted_iota(jnp.int32, (count, width), 1) // head_dim
    spread = [jnp.where(head_of == h, query, 0.0) for h in range(HEADS)]
    spread = jnp.concatenate(spread, axis=0).astype(BF16)
    scale = 1.0 / math.sqrt(head_dim)
    mapped[...] = (dot_last(spread, w_keyval[:, :width]) * scale).reshape(mapped.shape)

    def attend(g, score):
        limit = jnp.concatenate([limits[g]] * (slots // 128), axis=1)
        masked = jnp.where(key[...] < limit, score, -jnp.inf)
        exponent = jnp.exp(masked - jnp.max(masked, axis=-1, keepdims=True))
        values = dot(exponent.astype(BF16), normed[g])
        mass = jnp.concatenate([values[:, width:]] * (width // 128), axis=1)
        values = values[:, :width] / mass
        mix[:, pl.ds(g * GROUP, GROUP), :] = values.reshape(HEADS, GROUP, width)

    for g in range(2, groups):
        normalise(g)
    scores = []
    for g in range(groups):
        mine = mapped[:, pl.ds(g * GROUP, GROUP), :].reshape(rows, width).astype(BF16)
        scores.append(dot_last(mine, normed[g, :, :width]))
    for g in range(groups):
        attend(g, scores[g])
    mixed = dot(mix[...].reshape(HEADS * count, width).astype(BF16), w_keyval[:, width:])
    picked = mixed[:count]
    for h in range(1, HEADS):
        picked = jnp.where(head_of == h, mixed[h * count : (h + 1) * count], picked)
    residual_ref[...] = (tokens + dot(picked.astype(BF16), w_out[...])).astype(BF16)


def attend(layout, captions, weights):
    count, context, width = captions.shape
    groups = count // GROUP
    slots = -(-context * GROUP // 128) * 128
    flops = 2 * count * width * (5 * width + 2 * HEADS * slots)
    return pl.pallas_call(
        attend_kernel,
        out_shape=jax.ShapeDtypeStruct((count, width), BF16),
        in_specs=[pl.BlockSpec(memory_space=pltpu.SMEM)]
        + [pl.BlockSpec(memory_space=pltpu.VMEM)] * 4,
        out_specs=pl.BlockSpec(memory_space=pltpu.VMEM),
        scratch_shapes=[
            pltpu.VMEM((groups, slots, width + 128), BF16),
            pltpu.VMEM((HEADS, count, width), F32),
            pltpu.VMEM((HEADS, count, width), F32),
            pltpu.VMEM((GROUP * HEADS, slots), jnp.int32),
            pltpu.VMEM((groups, GROUP * HEADS, 128), jnp.int32),
        ],
        compiler_params=pltpu.CompilerParams(vmem_limit_bytes=20 * MIB),
        cost_estimate=pl.CostEstimate(
            flops=8 * flops,
            bytes_accessed=2 * captions.size + 8 * width * width,
            transcendentals=count * HEADS * slots,
        ),
        name="attend",
    )(layout, jnp.transpose(captions, (1, 0, 2)), *weights)


def unit_kernel(images, units):
    value = images[...].astype(F32)
    units[...] = (value * inverse_norm(value)).astype(BF16)


def unit_rows(images):
    return pl.pallas_call(
        unit_kernel,
        out_shape=jax.ShapeDtypeStruct(images.shape, BF16),
        in_specs=[pl.BlockSpec(memory_space=pltpu.VMEM)],
        out_specs=pl.BlockSpec(memory_space=pltpu.VMEM),
        compiler_params=pltpu.CompilerParams(vmem_limit_bytes=4 * MIB),
        cost_estimate=pl.CostEstimate(
            flops=UNIT_FLOPS, bytes_accessed=4 * images.size, transcendentals=0
        ),
        name="unit",
    )(images)


def forward_kernel(residual_ref, w_up, w_down, w_proj, units_ref, embed_ref):
    residual = residual_ref[...].astype(F32)
    inner = layer_norm(residual).astype(BF16)
    hidden = dot(inner, w_up[...])
    hidden = (0.5 * hidden * (1.0 + erf(hidden * math.sqrt(0.5)))).astype(BF16)
    final = residual + dot(hidden, w_down[...])
    pooled = layer_norm(final).astype(BF16)
    embed = dot(pooled, w_proj[...]).astype(BF16)
    embed_ref[...] = embed
    embed = embed.astype(F32)
    units_ref[...] = (embed * inverse_norm(embed)).astype(BF16)


def forward(residual, weights):
    result = jax.ShapeDtypeStruct((residual.shape[0], weights[2].shape[1]), BF16)
    size = sum(w.size for w in weights)
    return pl.pallas_call(
        forward_kernel,
        out_shape=(result, result),
        in_specs=[pl.BlockSpec(memory_space=pltpu.VMEM)] * 4,
        out_specs=(pl.BlockSpec(memory_space=pltpu.VMEM),) * 2,
        compiler_params=pltpu.CompilerParams(vmem_limit_bytes=8 * MIB),
        cost_estimate=pl.CostEstimate(
            flops=4 * residual.shape[0] * size, bytes_accessed=2 * size, transcendentals=0
        ),
        name="forward",
    )(residual, *weights)


def unit_grad(grad, value):
    inverse = inverse_norm(value)
    inner = jnp.sum(value * grad, axis=-1, keepdims=True)
    return grad * inverse - value * (inner * inverse * inverse * inverse)


def lse_steps(tile, rows_of, columns, after):
    total, width = rows_of.shape[0], columns.shape[0]

    def score_tile(i):
        return LOGIT_SCALE * dot_last(rows_of[pl.ds(i * tile, tile), :], columns[...])

    def step(i, s, carry):
        top, mass = carry
        peak = jnp.max(s, axis=1, keepdims=True)
        after(pl.ds(i * tile, tile), s, peak, jnp.sum(jnp.exp(s - peak), axis=1, keepdims=True))
        higher = jnp.maximum(top, jnp.max(s, axis=0, keepdims=True))
        mass = mass * jnp.exp(top - higher) + jnp.sum(jnp.exp(s - higher), axis=0, keepdims=True)
        return higher, mass

    ends = (jnp.full((1, width), -jnp.inf, F32), jnp.zeros((1, width), F32))
    if total // tile <= 4:
        score = score_tile(0)
        for i in range(total // tile):
            following = score_tile(i + 1) if i + 1 < total // tile else None
            ends = step(i, score, ends)
            score = following
    else:
        ends = lax.fori_loop(0, total // tile, lambda i, c: step(i, score_tile(i), c), ends)
    return ends[0] + jnp.log(ends[1])


def loss_kernel(
    images_a,
    images_b,
    texts_a,
    texts_b,
    images,
    embed,
    image_out,
    text_out,
    pictures,
    texts,
    sides,
    row_lse,
    *,
    tile,
):
    half = images_a.shape[0]
    count = images.shape[0]
    pictures[:half, :] = images_a[...]
    pictures[half:, :] = images_b[...]
    texts[:half, :] = texts_a[...]
    texts[half:, :] = texts_b[...]

    def after(rows, s, peak, mass):
        sides[rows, :] = s[:, :128]
        row_lse[rows, :] = jnp.broadcast_to(peak + jnp.log(mass), (tile, 128))

    column_lse = lse_steps(tile, pictures, texts, after)

    def product(weights, other):
        both = dot(jnp.concatenate(weights, axis=0), other[...])
        return (0.5 * LOGIT_SCALE) * (both[:count] + both[count:])

    score = LOGIT_SCALE * dot_last(pictures[:count, :], texts[...])
    weights = [
        jnp.exp(score - row_lse[:count, :1]).astype(BF16),
        jnp.exp(score - column_lse).astype(BF16),
    ]
    image_grad = product(weights, texts) - LOGIT_SCALE * texts[:count, :].astype(F32)
    side = sides[...]
    weights = [
        jnp.exp(side - row_lse[...]).T[:count].astype(BF16),
        jnp.exp(side - column_lse[:, :128]).T[:count].astype(BF16),
    ]
    text_grad = product(weights, pictures) - LOGIT_SCALE * pictures[:count, :].astype(F32)
    image_out[...] = unit_grad(image_grad, images[...].astype(F32))
    text_out[...] = unit_grad(text_grad, embed[...].astype(F32))


def loss(pictures, texts, images, embed):
    half, width = pictures[0].shape
    total = 2 * half
    result = jax.ShapeDtypeStruct(images.shape, F32)
    return pl.pallas_call(
        functools.partial(loss_kernel, tile=256),
        out_shape=(result, result),
        in_specs=[pl.BlockSpec(memory_space=pltpu.VMEM)] * 6,
        out_specs=(pl.BlockSpec(memory_space=pltpu.VMEM),) * 2,
        scratch_shapes=[
            pltpu.VMEM((total, width), BF16),
            pltpu.VMEM((total, width), BF16),
            pltpu.VMEM((total, 128), F32),
            pltpu.VMEM((total, 128), F32),
        ],
        compiler_params=pltpu.CompilerParams(vmem_limit_bytes=40 * MIB),
        cost_estimate=pl.CostEstimate(
            flops=2 * total * total * width,
            bytes_accessed=4 * total * width,
            transcendentals=2 * total * total,
        ),
        name="loss",
    )(*pictures, *texts, images, embed)


def exchange(value, mask):
    devices = range(lax.axis_size("dp"))
    return lax.ppermute(value, "dp", [(i, i ^ mask) for i in devices])


def digit_masks(devices):
    groups, high = [], devices
    while high > 2:
        low = max(high // 4, 2)
        groups.append([k * low for k in range(1, high // low)])
        high = low
    return groups


def gather(value):
    for masks in digit_masks(lax.axis_size("dp")):
        parts = []
        for mask in masks:
            parts.append(exchange(value, mask))
        value, *parts = lax.optimization_barrier((value, *parts))
        value = jnp.concatenate([value, *parts], axis=0)
    return value, exchange(value, 1)


def body(captions, layout, images, w_query, w_keyval, w_out, w_up, w_down, w_proj):
    image_units = unit_rows(images)
    pictures = gather(image_units)
    residual = attend(layout, captions, (w_query, w_keyval, w_out))
    text_units, embed = forward(residual, (w_up, w_down, w_proj))
    texts = gather(text_units)
    return loss(pictures, texts, images, embed)


def solution(mesh):
    return jax.shard_map(
        body,
        mesh=mesh,
        in_specs=(P("dp", None, None), P(), P("dp", None), P(), P(), P(), P(), P(), P()),
        out_specs=(P("dp", None), P("dp", None)),
        check_vma=False,
    )
```

```python
import functools
import math

import jax
import jax.numpy as jnp
from jax import lax
from jax.experimental import pallas as pl
from jax.experimental.pallas import tpu as pltpu
from jax.sharding import PartitionSpec as P


HEADS = 12
GROUP = 8
LOGIT_SCALE = 100.0
LOGIT_BITS = LOGIT_SCALE * math.log2(math.e)
EPS_NORM = 1e-05
EPS_UNIT = 1e-06
BF16 = jnp.bfloat16
F32 = jnp.float32
MIB = 1024 * 1024
TABLE_FLOPS = 4 * 10**9


def layer_norm(values):
    center = values - jnp.mean(values, axis=-1, keepdims=True)
    spread = jnp.mean(center * center, axis=-1, keepdims=True)
    return center * lax.rsqrt(spread + EPS_NORM)


def inverse_norm(values):
    return lax.rsqrt(jnp.sum(values * values, axis=-1, keepdims=True) + EPS_UNIT)


def dot(left, right):
    return jnp.dot(left, right, preferred_element_type=F32)


def dot_last(left, right):
    return lax.dot_general(left, right, (((1,), (1,)), ((), ())), preferred_element_type=F32)


def erf(x):
    x = jnp.clip(x, -3.832506856900711, 3.832506856900711)
    y = x * x
    top = jnp.full_like(x, 0.00022905065861350646)
    for c in (
        0.0034082910107109506,
        0.050955695062380861,
        0.18520832239976145,
        1.128379143519084,
    ):
        top = top * y + c
    bottom = jnp.full_like(x, -1.1791602954361697e-7)
    for c in (
        0.000023547966471313185,
        0.0010179625278914885,
        0.014070470171167667,
        0.11098505178285362,
        0.49746925110067538,
        1.0,
    ):
        bottom = bottom * y + c
    return x * top / bottom


def attend_kernel(
    layout, caps, key, w_query, w_keyval, w_out, residual_ref, normed, mapped, mix, limits
):
    context, count, width = caps.shape
    groups = count // GROUP
    slots = normed.shape[1]
    head_dim = width // HEADS
    base = lax.axis_index("dp") * count
    lengths = [layout[0, base + c] for c in range(count)]
    ends = [jnp.clip(length - 1, 0, context - 1) for length in lengths]

    rows = GROUP * HEADS
    owner = lax.broadcasted_iota(jnp.int32, (rows, 128), 0) % GROUP
    for g in range(groups):
        limit = jnp.full((rows, 128), 0, jnp.int32)
        for k in range(GROUP):
            limit = jnp.where(owner == k, lengths[g * GROUP + k], limit)
        limits[g] = limit
        normed[g, :, width:] = jnp.ones((slots, 128), BF16)
    pair = 2 * GROUP
    done = (context + 1) // 2 * pair

    def normalise(g):
        for t in range(context // 2):
            value = caps[pl.ds(2 * t, 2), pl.ds(g * GROUP, GROUP)].astype(F32).reshape(pair, width)
            normed[g, pl.ds(t * pair, pair), :width] = layer_norm(value).astype(BF16)
        if context % 2:
            tail = layer_norm(caps[context - 1, pl.ds(g * GROUP, GROUP)].astype(F32))
            tail = jnp.concatenate([tail, jnp.zeros((GROUP, width), F32)], axis=0)
            normed[g, pl.ds(context // 2 * pair, pair), :width] = tail.astype(BF16)
        if done < slots:
            normed[g, pl.ds(done, slots - done), :width] = jnp.zeros((slots - done, width), BF16)

    normalise(0)
    row = lax.broadcasted_iota(jnp.int32, (GROUP, width), 0)
    tokens = []
    for g in range(groups):
        part = pl.ds(g * GROUP, GROUP)
        lines = [caps[ends[g * GROUP + k], part].astype(F32) for k in range(GROUP)]
        token = lines[0]
        for k in range(1, GROUP):
            token = jnp.where(row == k, lines[k], token)
        tokens.append(token)
    tokens = jnp.concatenate(tokens, axis=0)
    end_normed = layer_norm(tokens).astype(BF16)
    query = dot(end_normed, w_query[...]).astype(BF16).astype(F32)
    normalise(1)
    head_of = lax.broadcasted_iota(jnp.int32, (count, width), 1) // head_dim
    spread = [jnp.where(head_of == h, query, 0.0) for h in range(HEADS)]
    spread = jnp.concatenate(spread, axis=0).astype(BF16)
    scale = 1.0 / math.sqrt(head_dim)
    mapped[...] = (dot_last(spread, w_keyval[:, :width]) * scale).reshape(mapped.shape)

    def attend(g, score):
        limit = jnp.concatenate([limits[g]] * (slots // 128), axis=1)
        masked = jnp.where(key[...] < limit, score, -jnp.inf)
        exponent = jnp.exp(masked - jnp.max(masked, axis=-1, keepdims=True))
        values = dot(exponent.astype(BF16), normed[g])
        mass = jnp.concatenate([values[:, width:]] * (width // 128), axis=1)
        values = values[:, :width] / mass
        mix[:, pl.ds(g * GROUP, GROUP), :] = values.reshape(HEADS, GROUP, width)

    for g in range(2, groups):
        normalise(g)
    scores = []
    for g in range(groups):
        mine = mapped[:, pl.ds(g * GROUP, GROUP), :].reshape(rows, width).astype(BF16)
        scores.append(dot_last(mine, normed[g, :, :width]))
    for g in range(groups):
        attend(g, scores[g])
    mixed = dot(mix[...].reshape(HEADS * count, width).astype(BF16), w_keyval[:, width:])
    picked = mixed[:count]
    for h in range(1, HEADS):
        picked = jnp.where(head_of == h, mixed[h * count : (h + 1) * count], picked)
    residual_ref[...] = (tokens + dot(picked.astype(BF16), w_out[...])).astype(BF16)


def slots_of(context):
    return -(-context * GROUP // 128) * 128


def table_kernel(key, *, context):
    lane = lax.broadcasted_iota(jnp.int32, key.shape, 1)
    line = lax.broadcasted_iota(jnp.int32, key.shape, 0)
    key[...] = jnp.where(lane % GROUP == line % GROUP, lane // GROUP, context)


def slot_table(context):
    return pl.pallas_call(
        functools.partial(table_kernel, context=context),
        out_shape=jax.ShapeDtypeStruct((GROUP * HEADS, slots_of(context)), jnp.int32),
        out_specs=pl.BlockSpec(memory_space=pltpu.VMEM),
        compiler_params=pltpu.CompilerParams(vmem_limit_bytes=4 * MIB),
        cost_estimate=pl.CostEstimate(flops=TABLE_FLOPS, bytes_accessed=0, transcendentals=0),
        name="table",
    )()


def attend(layout, captions, key, weights):
    count, context, width = captions.shape
    groups = count // GROUP
    slots = slots_of(context)
    flops = 2 * count * width * (5 * width + 2 * HEADS * slots)
    return pl.pallas_call(
        attend_kernel,
        out_shape=jax.ShapeDtypeStruct((count, width), BF16),
        in_specs=[pl.BlockSpec(memory_space=pltpu.SMEM)]
        + [pl.BlockSpec(memory_space=pltpu.VMEM)] * 5,
        out_specs=pl.BlockSpec(memory_space=pltpu.VMEM),
        scratch_shapes=[
            pltpu.VMEM((groups, slots, width + 128), BF16),
            pltpu.VMEM((HEADS, count, width), F32),
            pltpu.VMEM((HEADS, count, width), F32),
            pltpu.VMEM((groups, GROUP * HEADS, 128), jnp.int32),
        ],
        compiler_params=pltpu.CompilerParams(vmem_limit_bytes=20 * MIB),
        cost_estimate=pl.CostEstimate(
            flops=8 * flops,
            bytes_accessed=2 * captions.size + 8 * width * width,
            transcendentals=count * HEADS * slots,
        ),
        name="attend",
    )(layout, jnp.transpose(captions, (1, 0, 2)), key, *weights)


def forward_kernel(residual_ref, w_up, w_down, w_proj, units_ref, embed_ref):
    residual = residual_ref[...].astype(F32)
    inner = layer_norm(residual).astype(BF16)
    hidden = dot(inner, w_up[...])
    hidden = (0.5 * hidden * (1.0 + erf(hidden * math.sqrt(0.5)))).astype(BF16)
    final = residual + dot(hidden, w_down[...])
    pooled = layer_norm(final).astype(BF16)
    embed = dot(pooled, w_proj[...]).astype(BF16)
    embed_ref[...] = embed
    embed = embed.astype(F32)
    units_ref[...] = (embed * inverse_norm(embed)).astype(BF16)


def forward(residual, weights):
    result = jax.ShapeDtypeStruct((residual.shape[0], weights[2].shape[1]), BF16)
    size = sum(w.size for w in weights)
    return pl.pallas_call(
        forward_kernel,
        out_shape=(result, result),
        in_specs=[pl.BlockSpec(memory_space=pltpu.VMEM)] * 4,
        out_specs=(pl.BlockSpec(memory_space=pltpu.VMEM),) * 2,
        compiler_params=pltpu.CompilerParams(vmem_limit_bytes=8 * MIB),
        cost_estimate=pl.CostEstimate(
            flops=4 * residual.shape[0] * size, bytes_accessed=2 * size, transcendentals=0
        ),
        name="forward",
    )(residual, *weights)


def unit_grad(grad, value):
    inverse = inverse_norm(value)
    inner = jnp.sum(value * grad, axis=-1, keepdims=True)
    return grad * inverse - value * (inner * inverse * inverse * inverse)


def lse_steps(tile, rows_of, columns, after):
    total, width = rows_of.shape[0], columns.shape[0]

    def score_tile(i):
        return LOGIT_BITS * dot_last(rows_of[pl.ds(i * tile, tile), :], columns[...])

    def step(i, s, carry):
        top, mass = carry
        peak = jnp.max(s, axis=1, keepdims=True)
        after(pl.ds(i * tile, tile), s, peak, jnp.sum(jnp.exp2(s - peak), axis=1, keepdims=True))
        higher = jnp.maximum(top, jnp.max(s, axis=0, keepdims=True))
        mass = mass * jnp.exp2(top - higher) + jnp.sum(jnp.exp2(s - higher), axis=0, keepdims=True)
        return higher, mass

    ends = (jnp.full((1, width), -jnp.inf, F32), jnp.zeros((1, width), F32))
    if total // tile <= 4:
        score = score_tile(0)
        for i in range(total // tile):
            following = score_tile(i + 1) if i + 1 < total // tile else None
            ends = step(i, score, ends)
            score = following
    else:
        ends = lax.fori_loop(0, total // tile, lambda i, c: step(i, score_tile(i), c), ends)
    return ends[0] + jnp.log2(ends[1])


def unit_kernel(images_a, images_b, pictures, *, tile):
    half = images_a.shape[0]
    for h, part in enumerate((images_a, images_b)):
        for i in range(0, half, tile):
            value = part[i : i + tile, :].astype(F32)
            rows = pl.ds(h * half + i, tile)
            pictures[rows, :] = (value * inverse_norm(value)).astype(BF16)


def product(weights, other):
    return (0.5 * LOGIT_SCALE) * dot(weights.astype(BF16), other[...])


def near_kernel(
    pictures,
    texts_a,
    row_peak,
    row_mass,
    sides,
    own_scores,
    image_part,
    text_part,
    *,
    tile,
):
    count = own_scores.shape[0]

    def after(rows, s, peak, mass):
        sides[rows, :] = s[:, :128]
        row_peak[rows, :] = jnp.broadcast_to(peak, (tile, 128))
        row_mass[rows, :] = jnp.broadcast_to(mass, (tile, 128))

    lse = lse_steps(tile, pictures, texts_a, after)
    score = LOGIT_BITS * dot_last(pictures[:count, :], texts_a[...])
    own_scores[...] = score
    image_part[...] = product(jnp.exp2(score - lse), texts_a) - LOGIT_SCALE * texts_a[
        :count, :
    ].astype(F32)
    text_part[...] = product(
        jnp.exp2(sides[...] - lse[:, :128]).T[:count], pictures
    ) - LOGIT_SCALE * pictures[:count, :].astype(F32)


def far_kernel(
    pictures,
    texts_a,
    texts_b,
    row_peak,
    row_mass,
    sides,
    scores_a,
    image_part,
    text_part,
    images,
    embed,
    image_out,
    text_out,
    row_lse,
    *,
    tile,
):
    count = images.shape[0]

    def after(rows, s, peak, mass):
        near = row_peak[rows, :1]
        top = jnp.maximum(peak, near)
        mass = mass * jnp.exp2(peak - top) + row_mass[rows, :1] * jnp.exp2(near - top)
        row_lse[rows, :] = jnp.broadcast_to(top + jnp.log2(mass), (tile, 128))

    lse_b = lse_steps(tile, pictures, texts_b, after)
    lse = row_lse[:count, :1]
    scores_b = LOGIT_BITS * dot_last(pictures[:count, :], texts_b[...])
    both = product(
        jnp.concatenate([jnp.exp2(scores_b - lse), jnp.exp2(scores_b - lse_b)], axis=0), texts_b
    )
    image_grad = image_part[...] + both[:count] + both[count:]
    image_grad += product(jnp.exp2(scores_a[...] - lse), texts_a)
    weights = jnp.exp2(sides[...] - row_lse[...]).T[:count]
    text_grad = text_part[...] + product(weights, pictures)
    image_out[...] = unit_grad(image_grad, images[...].astype(F32))
    text_out[...] = unit_grad(text_grad, embed[...].astype(F32))


def cost(rows, columns, width):
    return pl.CostEstimate(
        flops=2 * rows * columns * width,
        bytes_accessed=2 * (rows + columns) * width,
        transcendentals=2 * rows * columns,
    )


def unit_rows(images_a, images_b):
    half, width = images_a.shape
    return pl.pallas_call(
        functools.partial(unit_kernel, tile=256),
        out_shape=jax.ShapeDtypeStruct((2 * half, width), BF16),
        in_specs=[pl.BlockSpec(memory_space=pltpu.VMEM)] * 2,
        out_specs=pl.BlockSpec(memory_space=pltpu.VMEM),
        compiler_params=pltpu.CompilerParams(vmem_limit_bytes=20 * MIB),
        cost_estimate=cost(half, 8, width),
        name="unit",
    )(images_a, images_b)


def near(pictures, texts, count):
    half, width = texts.shape
    total = 2 * half
    shape = jax.ShapeDtypeStruct
    return pl.pallas_call(
        functools.partial(near_kernel, tile=512),
        out_shape=(
            shape((total, 128), F32),
            shape((total, 128), F32),
            shape((total, 128), F32),
            shape((count, half), F32),
            shape((count, width), F32),
            shape((count, width), F32),
        ),
        in_specs=[pl.BlockSpec(memory_space=pltpu.VMEM)] * 2,
        out_specs=(pl.BlockSpec(memory_space=pltpu.VMEM),) * 6,
        compiler_params=pltpu.CompilerParams(vmem_limit_bytes=24 * MIB),
        cost_estimate=cost(total, half, width),
        name="near",
    )(pictures, texts)


def far(pictures, texts, known, images, embed):
    half, width = texts[0].shape
    result = jax.ShapeDtypeStruct(images.shape, F32)
    return pl.pallas_call(
        functools.partial(far_kernel, tile=512),
        out_shape=(result, result),
        in_specs=[pl.BlockSpec(memory_space=pltpu.VMEM)] * 11,
        out_specs=(pl.BlockSpec(memory_space=pltpu.VMEM),) * 2,
        scratch_shapes=[pltpu.VMEM((2 * half, 128), F32)],
        compiler_params=pltpu.CompilerParams(vmem_limit_bytes=24 * MIB),
        cost_estimate=cost(2 * half, half, width),
        name="far",
    )(pictures, *texts, *known, images, embed)


def exchange(value, mask):
    devices = range(lax.axis_size("dp"))
    even, odd = mask if isinstance(mask, tuple) else (mask, mask)
    return lax.ppermute(value, "dp", [(i, i ^ (odd if i % 2 else even)) for i in devices])


def digit_masks(devices):
    groups, high = [], devices
    while high > 2:
        low = max(high // 4, 2)
        groups.append([k * low for k in range(1, high // low)])
        high = low
    return groups


def image_masks(devices):
    return digit_masks(devices)


def text_masks(devices):
    groups = [
        [masks[k] for k in ((2, 0, 1) if p else (1, 2, 0))] if len(masks) == 3 else masks
        for p, masks in enumerate(digit_masks(devices))
    ]
    if len(groups) > 1 and len(groups[0]) == len(groups[1]):
        swapped = [groups[1], groups[0]] + groups[2:]
        groups = [list(zip(even, odd)) for even, odd in zip(groups, swapped)]
    return groups


def gather(value, groups):
    for masks in groups:
        parts = []
        for mask in masks:
            parts.append(exchange(value, mask))
        value, *parts = lax.optimization_barrier((value, *parts))
        value = jnp.concatenate([value, *parts], axis=0)
    return value, exchange(value, 1)


def body(captions, layout, images, w_query, w_keyval, w_out, w_up, w_down, w_proj):
    devices = lax.axis_size("dp")
    key = slot_table(captions.shape[1])
    pictures = gather(images, image_masks(devices))
    residual = attend(layout, captions, key, (w_query, w_keyval, w_out))
    text_units, embed = forward(residual, (w_up, w_down, w_proj))
    texts = gather(text_units, text_masks(devices))
    pictures = unit_rows(*pictures)
    known = near(pictures, texts[0], images.shape[0])
    return far(pictures, texts, known, images, embed)


def solution(mesh):
    return jax.shard_map(
        body,
        mesh=mesh,
        in_specs=(P("dp", None, None), P(), P("dp", None), P(), P(), P(), P(), P(), P()),
        out_specs=(P("dp", None), P("dp", None)),
        check_vma=False,
    )
```

```python
import functools
import math

import jax
import jax.numpy as jnp
from jax import lax
from jax.experimental import pallas as pl
from jax.experimental.pallas import tpu as pltpu
from jax.sharding import PartitionSpec as P


HEADS = 12
GROUP = 8
LOGIT_SCALE = 100.0
EPS_NORM = 1e-05
EPS_UNIT = 1e-06
BF16 = jnp.bfloat16
F32 = jnp.float32
MIB = 1024 * 1024
TABLE_FLOPS = 4 * 10**9


def layer_norm(values):
    center = values - jnp.mean(values, axis=-1, keepdims=True)
    spread = jnp.mean(center * center, axis=-1, keepdims=True)
    return center * lax.rsqrt(spread + EPS_NORM)


def inverse_norm(values):
    return lax.rsqrt(jnp.sum(values * values, axis=-1, keepdims=True) + EPS_UNIT)


def dot(left, right):
    return jnp.dot(left, right, preferred_element_type=F32)


def dot_last(left, right):
    return lax.dot_general(left, right, (((1,), (1,)), ((), ())), preferred_element_type=F32)


def erf(x):
    x = jnp.clip(x, -3.832506856900711, 3.832506856900711)
    y = x * x
    top = jnp.full_like(x, 0.00022905065861350646)
    for c in (
        0.0034082910107109506,
        0.050955695062380861,
        0.18520832239976145,
        1.128379143519084,
    ):
        top = top * y + c
    bottom = jnp.full_like(x, -1.1791602954361697e-7)
    for c in (
        0.000023547966471313185,
        0.0010179625278914885,
        0.014070470171167667,
        0.11098505178285362,
        0.49746925110067538,
        1.0,
    ):
        bottom = bottom * y + c
    return x * top / bottom


def attend_kernel(
    layout, caps, key, w_query, w_keyval, w_out, residual_ref, normed, mapped, mix, limits
):
    context, count, width = caps.shape
    groups = count // GROUP
    slots = normed.shape[1]
    head_dim = width // HEADS
    base = lax.axis_index("dp") * count
    lengths = [layout[0, base + c] for c in range(count)]
    ends = [jnp.clip(length - 1, 0, context - 1) for length in lengths]

    rows = GROUP * HEADS
    owner = lax.broadcasted_iota(jnp.int32, (rows, 128), 0) % GROUP
    for g in range(groups):
        limit = jnp.full((rows, 128), 0, jnp.int32)
        for k in range(GROUP):
            limit = jnp.where(owner == k, lengths[g * GROUP + k], limit)
        limits[g] = limit
        normed[g, :, width:] = jnp.ones((slots, 128), BF16)
    pair = 2 * GROUP
    done = (context + 1) // 2 * pair

    def normalise(g):
        for t in range(context // 2):
            value = caps[pl.ds(2 * t, 2), pl.ds(g * GROUP, GROUP)].astype(F32).reshape(pair, width)
            normed[g, pl.ds(t * pair, pair), :width] = layer_norm(value).astype(BF16)
        if context % 2:
            tail = layer_norm(caps[context - 1, pl.ds(g * GROUP, GROUP)].astype(F32))
            tail = jnp.concatenate([tail, jnp.zeros((GROUP, width), F32)], axis=0)
            normed[g, pl.ds(context // 2 * pair, pair), :width] = tail.astype(BF16)
        if done < slots:
            normed[g, pl.ds(done, slots - done), :width] = jnp.zeros((slots - done, width), BF16)

    normalise(0)
    row = lax.broadcasted_iota(jnp.int32, (GROUP, width), 0)
    tokens = []
    for g in range(groups):
        part = pl.ds(g * GROUP, GROUP)
        lines = [caps[ends[g * GROUP + k], part].astype(F32) for k in range(GROUP)]
        token = lines[0]
        for k in range(1, GROUP):
            token = jnp.where(row == k, lines[k], token)
        tokens.append(token)
    tokens = jnp.concatenate(tokens, axis=0)
    end_normed = layer_norm(tokens).astype(BF16)
    query = dot(end_normed, w_query[...]).astype(BF16).astype(F32)
    normalise(1)
    head_of = lax.broadcasted_iota(jnp.int32, (count, width), 1) // head_dim
    spread = [jnp.where(head_of == h, query, 0.0) for h in range(HEADS)]
    spread = jnp.concatenate(spread, axis=0).astype(BF16)
    scale = 1.0 / math.sqrt(head_dim)
    mapped[...] = (dot_last(spread, w_keyval[:, :width]) * scale).reshape(mapped.shape)

    def attend(g, score):
        limit = jnp.concatenate([limits[g]] * (slots // 128), axis=1)
        masked = jnp.where(key[...] < limit, score, -jnp.inf)
        exponent = jnp.exp(masked - jnp.max(masked, axis=-1, keepdims=True))
        values = dot(exponent.astype(BF16), normed[g])
        mass = jnp.concatenate([values[:, width:]] * (width // 128), axis=1)
        values = values[:, :width] / mass
        mix[:, pl.ds(g * GROUP, GROUP), :] = values.reshape(HEADS, GROUP, width)

    for g in range(2, groups):
        normalise(g)
    scores = []
    for g in range(groups):
        mine = mapped[:, pl.ds(g * GROUP, GROUP), :].reshape(rows, width).astype(BF16)
        scores.append(dot_last(mine, normed[g, :, :width]))
    for g in range(groups):
        attend(g, scores[g])
    mixed = dot(mix[...].reshape(HEADS * count, width).astype(BF16), w_keyval[:, width:])
    picked = mixed[:count]
    for h in range(1, HEADS):
        picked = jnp.where(head_of == h, mixed[h * count : (h + 1) * count], picked)
    residual_ref[...] = (tokens + dot(picked.astype(BF16), w_out[...])).astype(BF16)


def slots_of(context):
    return -(-context * GROUP // 128) * 128


def table_kernel(key, *, context):
    lane = lax.broadcasted_iota(jnp.int32, key.shape, 1)
    line = lax.broadcasted_iota(jnp.int32, key.shape, 0)
    key[...] = jnp.where(lane % GROUP == line % GROUP, lane // GROUP, context)


def slot_table(context):
    return pl.pallas_call(
        functools.partial(table_kernel, context=context),
        out_shape=jax.ShapeDtypeStruct((GROUP * HEADS, slots_of(context)), jnp.int32),
        out_specs=pl.BlockSpec(memory_space=pltpu.VMEM),
        compiler_params=pltpu.CompilerParams(vmem_limit_bytes=4 * MIB),
        cost_estimate=pl.CostEstimate(flops=TABLE_FLOPS, bytes_accessed=0, transcendentals=0),
        name="table",
    )()


def attend(layout, captions, key, weights):
    count, context, width = captions.shape
    groups = count // GROUP
    slots = slots_of(context)
    flops = 2 * count * width * (5 * width + 2 * HEADS * slots)
    return pl.pallas_call(
        attend_kernel,
        out_shape=jax.ShapeDtypeStruct((count, width), BF16),
        in_specs=[pl.BlockSpec(memory_space=pltpu.SMEM)]
        + [pl.BlockSpec(memory_space=pltpu.VMEM)] * 5,
        out_specs=pl.BlockSpec(memory_space=pltpu.VMEM),
        scratch_shapes=[
            pltpu.VMEM((groups, slots, width + 128), BF16),
            pltpu.VMEM((HEADS, count, width), F32),
            pltpu.VMEM((HEADS, count, width), F32),
            pltpu.VMEM((groups, GROUP * HEADS, 128), jnp.int32),
        ],
        compiler_params=pltpu.CompilerParams(vmem_limit_bytes=20 * MIB),
        cost_estimate=pl.CostEstimate(
            flops=8 * flops,
            bytes_accessed=2 * captions.size + 8 * width * width,
            transcendentals=count * HEADS * slots,
        ),
        name="attend",
    )(layout, jnp.transpose(captions, (1, 0, 2)), key, *weights)


def forward_kernel(residual_ref, w_up, w_down, w_proj, units_ref, embed_ref):
    residual = residual_ref[...].astype(F32)
    inner = layer_norm(residual).astype(BF16)
    hidden = dot(inner, w_up[...])
    hidden = (0.5 * hidden * (1.0 + erf(hidden * math.sqrt(0.5)))).astype(BF16)
    final = residual + dot(hidden, w_down[...])
    pooled = layer_norm(final).astype(BF16)
    embed = dot(pooled, w_proj[...]).astype(BF16)
    embed_ref[...] = embed
    embed = embed.astype(F32)
    units_ref[...] = (embed * inverse_norm(embed)).astype(BF16)


def forward(residual, weights):
    result = jax.ShapeDtypeStruct((residual.shape[0], weights[2].shape[1]), BF16)
    size = sum(w.size for w in weights)
    return pl.pallas_call(
        forward_kernel,
        out_shape=(result, result),
        in_specs=[pl.BlockSpec(memory_space=pltpu.VMEM)] * 4,
        out_specs=(pl.BlockSpec(memory_space=pltpu.VMEM),) * 2,
        compiler_params=pltpu.CompilerParams(vmem_limit_bytes=8 * MIB),
        cost_estimate=pl.CostEstimate(
            flops=4 * residual.shape[0] * size, bytes_accessed=2 * size, transcendentals=0
        ),
        name="forward",
    )(residual, *weights)


def unit_grad(grad, value):
    inverse = inverse_norm(value)
    inner = jnp.sum(value * grad, axis=-1, keepdims=True)
    return grad * inverse - value * (inner * inverse * inverse * inverse)


def lse_steps(tile, rows_of, columns, after):
    total, width = rows_of.shape[0], columns.shape[0]

    def score_tile(i):
        return LOGIT_SCALE * dot_last(rows_of[pl.ds(i * tile, tile), :], columns[...])

    def step(i, s, carry):
        top, mass = carry
        peak = jnp.max(s, axis=1, keepdims=True)
        after(pl.ds(i * tile, tile), s, peak, jnp.sum(jnp.exp(s - peak), axis=1, keepdims=True))
        higher = jnp.maximum(top, jnp.max(s, axis=0, keepdims=True))
        mass = mass * jnp.exp(top - higher) + jnp.sum(jnp.exp(s - higher), axis=0, keepdims=True)
        return higher, mass

    ends = (jnp.full((1, width), -jnp.inf, F32), jnp.zeros((1, width), F32))
    if total // tile <= 4:
        score = score_tile(0)
        for i in range(total // tile):
            following = score_tile(i + 1) if i + 1 < total // tile else None
            ends = step(i, score, ends)
            score = following
    else:
        ends = lax.fori_loop(0, total // tile, lambda i, c: step(i, score_tile(i), c), ends)
    return ends[0] + jnp.log(ends[1])


def near_kernel(
    images_a, images_b, texts_a, pictures, column_lse, row_peak, row_mass, sides, own_scores, *, tile
):
    half = images_a.shape[0]
    for h, part in enumerate((images_a, images_b)):
        for i in range(0, half, tile):
            value = part[i : i + tile, :].astype(F32)
            rows = pl.ds(h * half + i, tile)
            pictures[rows, :] = (value * inverse_norm(value)).astype(BF16)

    def after(rows, s, peak, mass):
        sides[rows, :] = s[:, :128]
        row_peak[rows, :] = jnp.broadcast_to(peak, (tile, 128))
        row_mass[rows, :] = jnp.broadcast_to(mass, (tile, 128))

    lse = lse_steps(tile, pictures, texts_a, after)
    column_lse[...] = jnp.broadcast_to(lse, column_lse.shape)
    own = pictures[: own_scores.shape[0], :]
    own_scores[...] = LOGIT_SCALE * dot_last(own, texts_a[...])


def far_kernel(
    pictures,
    texts_a,
    texts_b,
    lse_a,
    row_peak,
    row_mass,
    sides,
    scores_a,
    images,
    embed,
    image_out,
    text_out,
    row_lse,
    *,
    tile,
):
    count = images.shape[0]

    def after(rows, s, peak, mass):
        near = row_peak[rows, :1]
        top = jnp.maximum(peak, near)
        mass = mass * jnp.exp(peak - top) + row_mass[rows, :1] * jnp.exp(near - top)
        row_lse[rows, :] = jnp.broadcast_to(top + jnp.log(mass), (tile, 128))

    lse_b = lse_steps(tile, pictures, texts_b, after)
    lse_a = lse_a[:1, :]

    def product(weights, other):
        both = dot(jnp.concatenate(weights, axis=0).astype(BF16), other[...])
        return (0.5 * LOGIT_SCALE) * (both[:count] + both[count:])

    lse = row_lse[:count, :1]
    scores_b = LOGIT_SCALE * dot_last(pictures[:count, :], texts_b[...])
    image_grad = -LOGIT_SCALE * texts_a[:count, :].astype(F32)
    for score, line, texts in ((scores_a[...], lse_a, texts_a), (scores_b, lse_b, texts_b)):
        image_grad += product([jnp.exp(score - lse), jnp.exp(score - line)], texts)
    side = sides[...]
    weights = [
        jnp.exp(side - row_lse[...]).T[:count],
        jnp.exp(side - lse_a[:, :128]).T[:count],
    ]
    text_grad = product(weights, pictures) - LOGIT_SCALE * pictures[:count, :].astype(F32)
    image_out[...] = unit_grad(image_grad, images[...].astype(F32))
    text_out[...] = unit_grad(text_grad, embed[...].astype(F32))


def cost(rows, columns, width):
    return pl.CostEstimate(
        flops=2 * rows * columns * width,
        bytes_accessed=2 * (rows + columns) * width,
        transcendentals=2 * rows * columns,
    )


def near(pictures, texts, count):
    half, width = texts.shape
    total = 2 * half
    shape = jax.ShapeDtypeStruct
    return pl.pallas_call(
        functools.partial(near_kernel, tile=512),
        out_shape=(
            shape((total, width), BF16),
            shape((8, half), F32),
            shape((total, 128), F32),
            shape((total, 128), F32),
            shape((total, 128), F32),
            shape((count, half), F32),
        ),
        in_specs=[pl.BlockSpec(memory_space=pltpu.VMEM)] * 3,
        out_specs=(pl.BlockSpec(memory_space=pltpu.VMEM),) * 6,
        compiler_params=pltpu.CompilerParams(vmem_limit_bytes=24 * MIB),
        cost_estimate=cost(total, half, width),
        name="near",
    )(*pictures, texts)


def far(known, texts, images, embed):
    pictures, column_lse, row_peak, row_mass, sides, own_scores = known
    half, width = texts[0].shape
    result = jax.ShapeDtypeStruct(images.shape, F32)
    return pl.pallas_call(
        functools.partial(far_kernel, tile=512),
        out_shape=(result, result),
        in_specs=[pl.BlockSpec(memory_space=pltpu.VMEM)] * 10,
        out_specs=(pl.BlockSpec(memory_space=pltpu.VMEM),) * 2,
        scratch_shapes=[pltpu.VMEM((2 * half, 128), F32)],
        compiler_params=pltpu.CompilerParams(vmem_limit_bytes=24 * MIB),
        cost_estimate=cost(2 * half, half, width),
        name="far",
    )(pictures, *texts, column_lse, row_peak, row_mass, sides, own_scores, images, embed)


def exchange(value, mask):
    devices = range(lax.axis_size("dp"))
    even, odd = mask if isinstance(mask, tuple) else (mask, mask)
    return lax.ppermute(value, "dp", [(i, i ^ (odd if i % 2 else even)) for i in devices])


def digit_masks(devices):
    groups, high = [], devices
    while high > 2:
        low = max(high // 4, 2)
        groups.append([k * low for k in range(1, high // low)])
        high = low
    return groups


def image_masks(devices):
    return digit_masks(devices)


def text_masks(devices):
    groups = [
        [masks[k] for k in ((2, 0, 1) if p else (1, 2, 0))] if len(masks) == 3 else masks
        for p, masks in enumerate(digit_masks(devices))
    ]
    if len(groups) > 1 and len(groups[0]) == len(groups[1]):
        swapped = [groups[1], groups[0]] + groups[2:]
        groups = [list(zip(even, odd)) for even, odd in zip(groups, swapped)]
    return groups


def gather(value, groups):
    for masks in groups:
        parts = []
        for mask in masks:
            parts.append(exchange(value, mask))
        value, *parts = lax.optimization_barrier((value, *parts))
        value = jnp.concatenate([value, *parts], axis=0)
    return value, exchange(value, 1)


def body(captions, layout, images, w_query, w_keyval, w_out, w_up, w_down, w_proj):
    devices = lax.axis_size("dp")
    key = slot_table(captions.shape[1])
    pictures = gather(images, image_masks(devices))
    residual = attend(layout, captions, key, (w_query, w_keyval, w_out))
    text_units, embed = forward(residual, (w_up, w_down, w_proj))
    texts = gather(text_units, text_masks(devices))
    known = near(pictures, texts[0], images.shape[0])
    return far(known, texts, images, embed)


def solution(mesh):
    return jax.shard_map(
        body,
        mesh=mesh,
        in_specs=(P("dp", None, None), P(), P("dp", None), P(), P(), P(), P(), P(), P()),
        out_specs=(P("dp", None), P("dp", None)),
        check_vma=False,
    )
```
